32 devices in a mesh: model: 8 (over z, y), fsdp: 4 (over x, core).
Axes of the slice: x: 2, y: 2, z: 4, core: 2. Of those that a mesh axis runs over, the one named last changes fastest.
Arguments:
- tok_ids: int32 [4, 1024], P('fsdp')
- tok_labels: int32 [4, 1024], P('fsdp')
- emb_table: bfloat16 [151936, 896], P(('model', 'fsdp'))
- w_gate: bfloat16 [896, 4864], P('fsdp')
- w_up: bfloat16 [896, 4864], P('fsdp')
- w_down: bfloat16 [4864, 896], P('fsdp')
- gain_in: float32 [896], replicated
- gain_out: float32 [896], replicated
Outputs:
- output 1: float32 [], replicated
- output 2: float32 [151936, 896], P(('model', 'fsdp'))
- output 3: float32 [896, 4864], P('fsdp')
- output 4: float32 [896, 4864], P('fsdp')
- output 5: float32 [4864, 896], P('fsdp')
All inputs are finite; a program needn't handle non-finite values.
Results may differ from the reference program's by a relative error of at most 0.0111091.
Values are sent between devices in bfloat16 or wider.
A program may use at most 1 GiB of HBM per device.

```python
import jax
import jax.numpy as jnp
from jax import lax

V = 151936
D = 896
F = 4864
BATCH = 4
SEQ = 1024
HEAD_BLOCK = 64
EPS = 1e-6


def draw_tokens(base_key):
    id_key, label_key = jax.random.split(base_key)
    tok_ids = jax.random.randint(id_key, (BATCH, SEQ), 0, V, dtype=jnp.int32)
    tok_ids = tok_ids.at[0, 0].set(0).at[BATCH - 1, SEQ - 1].set(V - 1)
    tok_labels = jax.random.randint(label_key, (BATCH, SEQ), 0, V, dtype=jnp.int32)
    tok_labels = tok_labels.at[0, 0].set(V - 1).at[BATCH - 1, SEQ - 1].set(0)
    return tok_ids, tok_labels


def setup_inputs(seed: int = 0) -> dict:
    rng_keys = jax.random.split(jax.random.key(seed), 7)
    tok_ids, tok_labels = draw_tokens(rng_keys[0])
    emb_table = (jax.random.normal(rng_keys[1], (V, D), jnp.float32) * D ** -0.5).astype(jnp.bfloat16)
    w_gate = (jax.random.normal(rng_keys[2], (D, F), jnp.float32) * D ** -0.5).astype(jnp.bfloat16)
    w_up = (jax.random.normal(rng_keys[3], (D, F), jnp.float32) * D ** -0.5).astype(jnp.bfloat16)
    w_down = (jax.random.normal(rng_keys[4], (F, D), jnp.float32) * (2.0 * (F * D) ** -0.5)).astype(jnp.bfloat16)
    gain_in = jax.random.uniform(rng_keys[5], (D,), jnp.float32, 0.5, 1.5)
    gain_out = jax.random.uniform(rng_keys[6], (D,), jnp.float32, 0.5, 1.5)
    return {"tok_ids": tok_ids, "tok_labels": tok_labels, "emb_table": emb_table, "w_gate": w_gate, "w_up": w_up, "w_down": w_down, "gain_in": gain_in, "gain_out": gain_out}


def rms_scale(values, gain_vec):
    mean_sq = jnp.mean(values * values, axis=-1, keepdims=True)
    return values * lax.rsqrt(mean_sq + EPS) * gain_vec


def reference(tok_ids, tok_labels, emb_table, w_gate, w_up, w_down, gain_in, gain_out):
    num_tokens = BATCH * SEQ
    flat_ids = tok_ids.reshape(num_tokens)
    flat_labels = tok_labels.reshape(num_tokens)
    x_emb = emb_table[flat_ids].astype(jnp.float32)
    normed_in, norm_in_back = jax.vjp(lambda values: rms_scale(values, gain_in), x_emb)
    normed_bf = normed_in.astype(jnp.bfloat16)
    gate_f = jnp.dot(normed_bf, w_gate, preferred_element_type=jnp.float32).astype(jnp.bfloat16).astype(jnp.float32)
    up_f = jnp.dot(normed_bf, w_up, preferred_element_type=jnp.float32).astype(jnp.bfloat16).astype(jnp.float32)
    gate_sig = jax.nn.sigmoid(gate_f)
    silu_gate = gate_f * gate_sig
    act_bf = (silu_gate * up_f).astype(jnp.bfloat16)
    mlp_out = jnp.dot(act_bf, w_down, preferred_element_type=jnp.float32).astype(jnp.bfloat16)
    h_res = x_emb + mlp_out.astype(jnp.float32)
    hn_f, norm_out_back = jax.vjp(lambda values: rms_scale(values, gain_out), h_res)
    hn_bf = hn_f.astype(jnp.bfloat16)
    num_blocks = num_tokens // HEAD_BLOCK
    hn_blocks = hn_bf.reshape(num_blocks, HEAD_BLOCK, D)
    label_blocks = flat_labels.reshape(num_blocks, HEAD_BLOCK)

    def head_step(d_head, block_in):
        hn_blk, label_blk = block_in
        logits = jnp.dot(hn_blk, emb_table.T, preferred_element_type=jnp.float32)
        row_max = jnp.max(logits, axis=-1, keepdims=True)
        exp_shift = jnp.exp(logits - row_max)
        sum_exp = jnp.sum(exp_shift, axis=-1, keepdims=True)
        onehot = lax.broadcasted_iota(jnp.int32, logits.shape, 1) == label_blk[:, None]
        label_logit = jnp.sum(jnp.where(onehot, logits, 0.0), axis=-1)
        tok_loss = row_max[:, 0] + jnp.log(sum_exp[:, 0]) - label_logit
        soft_probs = exp_shift / sum_exp
        d_logits = (jnp.where(onehot, soft_probs - 1.0, soft_probs) / num_tokens).astype(jnp.bfloat16)
        d_head = d_head + jnp.dot(d_logits.T, hn_blk, preferred_element_type=jnp.float32)
        d_hn = jnp.dot(d_logits, emb_table, preferred_element_type=jnp.float32)
        return d_head, (tok_loss, d_hn)

    d_head, (tok_losses, d_hn_blocks) = lax.scan(head_step, jnp.zeros((V, D), jnp.float32), (hn_blocks, label_blocks))
    loss = jnp.sum(tok_losses) / num_tokens
    d_hn = d_hn_blocks.reshape(num_tokens, D)
    d_hidden = norm_out_back(d_hn)[0]
    d_mlp = d_hidden.astype(jnp.bfloat16)
    d_act = jnp.dot(d_mlp, w_down.T, preferred_element_type=jnp.float32)
    grad_down = jnp.dot(act_bf.T, d_mlp, preferred_element_type=jnp.float32)
    d_gate = (d_act * up_f * (gate_sig * (1.0 + gate_f * (1.0 - gate_sig)))).astype(jnp.bfloat16)
    d_up = (d_act * silu_gate).astype(jnp.bfloat16)
    grad_gate = jnp.dot(normed_bf.T, d_gate, preferred_element_type=jnp.float32)
    grad_up = jnp.dot(normed_bf.T, d_up, preferred_element_type=jnp.float32)
    d_normed = jnp.dot(d_gate, w_gate.T, preferred_element_type=jnp.float32) + jnp.dot(d_up, w_up.T, preferred_element_type=jnp.float32)
    d_x = d_hidden + norm_in_back(d_normed)[0]
    d_in = jax.ops.segment_sum(d_x, flat_ids, num_segments=V)
    grad_table = d_head + d_in
    return (loss, grad_table, grad_gate, grad_up, grad_down)
```

```python
import functools

import jax
import jax.numpy as jnp
from jax import lax
from jax.experimental import pallas as pl
from jax.experimental.pallas import tpu as pltpu
from jax.sharding import PartitionSpec as P

EPS = 1e-6
ALL = ("model", "fsdp")
SMEM = pltpu.MemorySpace.SMEM
BF = jnp.bfloat16
F32 = jnp.float32


def rms_scale(values, gain_vec):
    mean_sq = jnp.mean(values * values, axis=-1, keepdims=True)
    return values * lax.rsqrt(mean_sq + EPS) * gain_vec


def mlp_forward(x_emb, gain_in, w_gate, w_up, w_down):
    normed_in, norm_in_back = jax.vjp(lambda values: rms_scale(values, gain_in), x_emb)
    normed_bf = normed_in.astype(BF)
    gate_f = jnp.dot(normed_bf, w_gate, preferred_element_type=F32).astype(BF).astype(F32)
    up_f = jnp.dot(normed_bf, w_up, preferred_element_type=F32).astype(BF).astype(F32)
    gate_sig = jax.nn.sigmoid(gate_f)
    silu_gate = gate_f * gate_sig
    act_bf = (silu_gate * up_f).astype(BF)
    mlp_out = jnp.dot(act_bf, w_down, preferred_element_type=F32).astype(BF)
    h_res = x_emb + mlp_out.astype(F32)
    return h_res, (norm_in_back, normed_bf, gate_f, up_f, gate_sig, silu_gate)


def gather_rows(ids, base, table, table_tail):
    total = ids.shape[0]
    rows, width = table.shape
    depth = 64
    last_block = rows // 8 * 8

    def kernel(ids_ref, base_ref, table_ref, tail_ref, out_ref, token, held, wide, in_sem):
        start_row = base_ref[0]

        def scan(group, filled):
            for k in range(8):
                t = group * 8 + k
                row = ids_ref[t] - start_row
                token[filled] = t
                filled = filled + ((row >= 0) & (row < rows)).astype(jnp.int32)
            return filled

        filled = lax.fori_loop(0, total // 8, scan, 0)

        def row_of(j):
            return ids_ref[token[j]] - start_row

        def block_copy(j):
            block = jnp.minimum(row_of(j) // 8 * 8, last_block - 8)
            slot = lax.rem(j, depth)
            return pltpu.make_async_copy(table_ref.at[pl.ds(pl.multiple_of(block, 8), 8)], held.at[slot], in_sem.at[slot])

        def begin(j, _):
            block_copy(j).start()
            return 0

        lax.fori_loop(0, jnp.minimum(filled, depth), begin, 0)

        def clear(i, _):
            wide[pl.ds(pl.multiple_of(i * 64, 64), 64), :] = jnp.zeros((64, width), F32)
            return 0

        lax.fori_loop(0, total // 64, clear, 0)
        sublane = lax.broadcasted_iota(jnp.int32, (8, width), 0)

        def step(j, _):
            block_copy(j).wait()
            row = row_of(j)
            body = held[lax.rem(j, depth)].astype(F32)
            tail = tail_ref[...].astype(F32)
            in_tail = row >= last_block
            chosen = jnp.where(in_tail, row - (rows - 8), row - row // 8 * 8)
            block = jnp.where(in_tail, tail, body)
            wide[pl.ds(token[j], 1), :] = jnp.sum(jnp.where(sublane == chosen, block, 0.0), axis=0, keepdims=True)

            @pl.when(j + depth < filled)
            def _():
                block_copy(j + depth).start()

            return 0

        lax.fori_loop(0, filled, step, 0)

        def narrow(i, _):
            where = pl.ds(pl.multiple_of(i * 64, 64), 64)
            out_ref[where, :] = wide[where, :].astype(BF)
            return 0

        lax.fori_loop(0, total // 64, narrow, 0)

    smem = pl.BlockSpec(memory_space=SMEM)
    return pl.pallas_call(
        kernel,
        out_shape=jax.ShapeDtypeStruct((total, width), BF),
        in_specs=[smem, smem, pl.BlockSpec(memory_space=pl.ANY), pl.BlockSpec(memory_space=pltpu.VMEM)],
        out_specs=pl.BlockSpec(memory_space=pltpu.VMEM),
        scratch_shapes=[
            pltpu.SMEM((total + 8,), jnp.int32),
            pltpu.VMEM((depth, 8, width), BF),
            pltpu.VMEM((total + 8, width), F32),
            pltpu.SemaphoreType.DMA((depth,)),
        ],
        cost_estimate=pl.CostEstimate(flops=total * width * 100, bytes_accessed=total * width * 2, transcendentals=0),
        name="gather_rows",
    )(ids, base, table, table_tail)


def add_rows(ids, base, values, grad):
    total = ids.shape[0]
    rows, width = grad.shape
    block_rows = 512
    blocks = pl.cdiv(rows, block_rows)

    def kernel(ids_ref, base_ref, values_ref, grad_ref, out_ref, head, following, token, held, sem):
        block = pl.program_id(0)
        fetch = pltpu.make_async_copy(values_ref, held.at[pl.ds(0, total)], sem)

        @pl.when(block == 0)
        def _():
            fetch.start()
            start_row = base_ref[0]

            def clear(b, _):
                head[b] = -1
                return 0

            lax.fori_loop(0, blocks, clear, 0)

            def scan(group, filled):
                for k in range(8):
                    t = group * 8 + k
                    row = ids_ref[t] - start_row
                    token[filled] = t
                    filled = filled + ((row >= 0) & (row < rows)).astype(jnp.int32)
                return filled

            filled = lax.fori_loop(0, total // 8, scan, 0)

            def chain(j, _):
                owner = (ids_ref[token[j]] - start_row) // block_rows
                following[j] = head[owner]
                head[owner] = j
                return 0

            lax.fori_loop(0, filled, chain, 0)
            fetch.wait()

        out_ref[...] = grad_ref[...]
        block_start = base_ref[0] + block * block_rows
        sublane = lax.broadcasted_iota(jnp.int32, (8, width), 0)

        def add(j):
            t = token[j]
            row = ids_ref[t] - block_start
            where = pl.ds(pl.multiple_of(row // 8 * 8, 8), 8)
            out_ref[where, :] += jnp.where(sublane == row - row // 8 * 8, held[pl.ds(t, 1), :], 0.0)
            return following[j]

        lax.while_loop(lambda j: j >= 0, add, head[block])

    smem = pl.BlockSpec(memory_space=SMEM)
    block_spec = pl.BlockSpec((block_rows, width), lambda i: (i, 0))
    return pl.pallas_call(
        kernel,
        grid=(blocks,),
        out_shape=jax.ShapeDtypeStruct(grad.shape, F32),
        in_specs=[smem, smem, pl.BlockSpec(memory_space=pl.ANY), block_spec],
        out_specs=block_spec,
        scratch_shapes=[
            pltpu.SMEM((blocks,), jnp.int32),
            pltpu.SMEM((total,), jnp.int32),
            pltpu.SMEM((total + 8,), jnp.int32),
            pltpu.VMEM((total + 8, width), F32),
            pltpu.SemaphoreType.DMA,
        ],
        input_output_aliases={3: 0},
        cost_estimate=pl.CostEstimate(flops=total * width * 100, bytes_accessed=rows * width * 8, transcendentals=0),
        name="add_rows",
    )(ids, base, values, grad)


def solution(mesh):
    model_size, fsdp_size = mesh.shape["model"], mesh.shape["fsdp"]
    size = model_size * fsdp_size
    tok_spec = P("fsdp", None)
    row_spec = P(("model", "fsdp"), None)
    weight_spec = P("fsdp", None)

    def device_step(tok_ids, tok_labels, table, gate_shard, up_shard, down_shard, gain_in, gain_out):
        model_at, fsdp_at = lax.axis_index("model"), lax.axis_index("fsdp")
        me = model_at * fsdp_size + fsdp_at
        core, side = fsdp_at % 2, fsdp_at // 2
        local_count = tok_ids.shape[0] * tok_ids.shape[1]
        num_tokens = local_count * fsdp_size
        rows, width = table.shape
        hidden = gate_shard.shape[1]
        quarter, half = hidden // 4, hidden // 2

        both = jnp.stack([tok_ids.reshape(local_count), tok_labels.reshape(local_count)])
        both = lax.all_gather(both, "fsdp", axis=1, tiled=True)
        ids, labels = both[0], both[1]
        base = jnp.full((1,), me * rows, jnp.int32)
        x_emb = gather_rows(ids, base, table, table[rows - 8 :])
        x_emb = lax.psum_scatter(x_emb, ALL, scatter_dimension=0, tiled=True).astype(F32)

        w_gate = lax.all_gather(gate_shard, "fsdp", axis=0, tiled=True)
        w_up = lax.all_gather(up_shard, "fsdp", axis=0, tiled=True)
        w_down = lax.all_gather(down_shard, "fsdp", axis=0, tiled=True)

        h_res, (norm_in_back, a_mine, gate_f, up_f, gate_sig, silu_gate) = mlp_forward(x_emb, gain_in, w_gate, w_up, w_down)
        hn_f, norm_out_back = jax.vjp(lambda values: rms_scale(values, gain_out), h_res)
        hn = lax.all_gather(hn_f.astype(BF), ALL, axis=0, tiled=True)
        a_all = lax.all_gather(a_mine, ALL, axis=0, tiled=True)

        logits = jnp.einsum("td,vd->tv", hn, table, preferred_element_type=F32)
        row_max = lax.pmax(jnp.max(logits, axis=-1), ALL)
        exp_shift = jnp.exp(logits - row_max[:, None])
        local_labels = labels - me * rows
        onehot = lax.broadcasted_iota(jnp.int32, logits.shape, 1) == local_labels[:, None]
        part_stats = jnp.stack([jnp.sum(exp_shift, axis=-1), jnp.sum(jnp.where(onehot, logits, 0.0), axis=-1)])
        tok_stats = lax.psum(part_stats, ALL)
        sum_exp = tok_stats[0]
        tok_loss = row_max + jnp.log(sum_exp) - tok_stats[1]
        loss = jnp.sum(tok_loss) / num_tokens
        soft_probs = exp_shift / sum_exp[:, None]
        d_logits = (jnp.where(onehot, soft_probs - 1.0, soft_probs) / num_tokens).astype(BF)
        d_hn = jnp.einsum("tv,vd->td", d_logits, table, preferred_element_type=F32)
        d_hn = lax.psum_scatter(d_hn, ALL, scatter_dimension=0, tiled=True)
        d_head = jnp.einsum("tv,td->vd", d_logits, hn, preferred_element_type=F32)

        d_hidden = norm_out_back(d_hn)[0]
        d_mlp = d_hidden.astype(BF)
        d_act = jnp.einsum("td,fd->tf", d_mlp, w_down, preferred_element_type=F32)
        d_gate = (d_act * up_f * (gate_sig * (1.0 + gate_f * (1.0 - gate_sig)))).astype(BF)
        d_up = (d_act * silu_gate).astype(BF)
        d_normed = jnp.einsum("tf,df->td", d_gate, w_gate, preferred_element_type=F32) + jnp.einsum("tf,df->td", d_up, w_up, preferred_element_type=F32)
        d_x = d_hidden + norm_in_back(d_normed)[0]
        d_x_all = lax.all_gather(d_x, ALL, axis=0, tiled=True)
        grad_table = add_rows(ids, base, d_x_all, d_head)

        dm_all = lax.all_gather(d_mlp, ALL, axis=0, tiled=True)
        pick = lambda w: lax.dynamic_index_in_dim(w.reshape(width, 2, 2, quarter), core, axis=2, keepdims=False).reshape(width, half)
        gate_half, up_half = pick(w_gate), pick(w_up)
        down_half = lax.dynamic_index_in_dim(w_down.reshape(2, 2, quarter, width), core, axis=1, keepdims=False).reshape(half, width)
        gate_a = jnp.dot(a_all, gate_half, preferred_element_type=F32).astype(BF).astype(F32)
        up_a = jnp.dot(a_all, up_half, preferred_element_type=F32).astype(BF).astype(F32)
        sig_a = jax.nn.sigmoid(gate_a)
        silu_a = gate_a * sig_a
        act_a = (silu_a * up_a).astype(BF)
        d_act_a = jnp.einsum("td,fd->tf", dm_all, down_half, preferred_element_type=F32)
        d_gate_a = (d_act_a * up_a * (sig_a * (1.0 + gate_a * (1.0 - sig_a)))).astype(BF)
        d_up_a = (d_act_a * silu_a).astype(BF)
        chip_rows = width // 2
        a_chip = lax.dynamic_slice(a_all, (0, side * chip_rows), (num_tokens, chip_rows))
        act_own = lax.dynamic_slice(act_a, (0, side * quarter), (num_tokens, quarter))
        grad_down = jnp.einsum("tf,td->fd", act_own, dm_all, preferred_element_type=F32)
        swap = [(i, i ^ 1) for i in range(fsdp_size)]

        def finish(d_part):
            grad = jnp.einsum("td,tf->df", a_chip, d_part, preferred_element_type=F32)
            grad = grad.reshape(2, chip_rows // 2, half)
            kept = lax.dynamic_index_in_dim(grad, core, axis=0, keepdims=False)
            got = lax.ppermute(lax.dynamic_index_in_dim(grad, 1 - core, axis=0, keepdims=False), "fsdp", swap)
            low = jnp.where(core == 0, kept, got).reshape(chip_rows // 2, 2, 1, quarter)
            high = jnp.where(core == 0, got, kept).reshape(chip_rows // 2, 2, 1, quarter)
            return jnp.concatenate([low, high], axis=2).reshape(chip_rows // 2, hidden)

        return loss, grad_table, finish(d_gate_a), finish(d_up_a), grad_down

    return jax.shard_map(device_step, mesh=mesh, in_specs=(tok_spec, tok_spec, row_spec, weight_spec, weight_spec, weight_spec, P(), P()), out_specs=(P(), row_spec, weight_spec, weight_spec, weight_spec), check_vma=False)
```

```python
import jax
import jax.numpy as jnp
from jax import lax
from jax.experimental import pallas as pl
from jax.experimental.pallas import tpu as pltpu
from jax.sharding import PartitionSpec as P

EPS = 1e-6
ALL = ("model", "fsdp")
BF = jnp.bfloat16
F32 = jnp.float32
DMA = pltpu.SemaphoreType.DMA
VMEM = pltpu.VMEM
LANES, SUBLANES = 128, 8
DEPTH, LAST_Z = 4, 3
PAIR = (0, 1)
AWAY = (1, 2, 3)
FAR_FIRST = (3, 0, 2, 1)
SIDES = ((1, 1), (0, 1), (1, 0), (0, 0))
DEVICES, CHIPS = 32, 16
IN_SMEM = pl.BlockSpec(memory_space=pltpu.MemorySpace.SMEM)
IN_VMEM = pl.BlockSpec(memory_space=pltpu.MemorySpace.VMEM)
IN_PLACE = pl.BlockSpec(memory_space=pl.ANY)


def rows_at(i, n):
    return pl.ds(pl.multiple_of(i * n, n), n)


def repeat(count, body):
    lax.fori_loop(0, count, lambda i, c: body(i) or c, 0)


def iota(shape, dim):
    return lax.broadcasted_iota(jnp.int32, shape, dim)


def matmul(a, b):
    return jnp.dot(a, b, preferred_element_type=F32)


def matmul_nt(a, b):
    return jnp.einsum("ac,bc->ab", a, b, preferred_element_type=F32)


def whole(array):
    return pl.BlockSpec(array.shape, lambda *_: (0,) * array.ndim, pipeline_mode=pl.Buffered(1))


def rms_scale(values, gain_vec):
    mean_sq = jnp.mean(values * values, axis=-1, keepdims=True)
    return values * lax.rsqrt(mean_sq + EPS) * gain_vec


def mlp_forward(x_emb, gain_in, w_gate, w_up, w_down):
    normed_in, norm_in_back = jax.vjp(lambda values: rms_scale(values, gain_in), x_emb)
    normed_bf = normed_in.astype(BF)
    gate_f = matmul(normed_bf, w_gate).astype(BF).astype(F32)
    up_f = matmul(normed_bf, w_up).astype(BF).astype(F32)
    gate_sig = jax.nn.sigmoid(gate_f)
    silu_gate = gate_f * gate_sig
    act_bf = (silu_gate * up_f).astype(BF)
    mlp_out = matmul(act_bf, w_down).astype(BF)
    h_res = x_emb + mlp_out.astype(F32)
    return h_res, (norm_in_back, normed_bf, gate_f, up_f, gate_sig, silu_gate)


class Place:
    def __init__(self):
        self.model, self.fsdp = lax.axis_index("model"), lax.axis_index("fsdp")
        self.z, self.y = self.model // 2, self.model % 2
        self.x, self.core = self.fsdp // 2, self.fsdp % 2
        self.has_above, self.has_below = self.z < LAST_Z, self.z > 0
        self.over_y = self.device(self.model + 1 - 2 * self.y, self.fsdp)
        self.over_x = self.device(self.model, self.fsdp + 2 - DEPTH * self.x)
        self.over_core = self.device(self.model, self.fsdp + 1 - 2 * self.core)
        self.above = self.device(self.model + 2 * self.has_above, self.fsdp)
        self.below = self.device(self.model - 2 * self.has_below, self.fsdp)

    def device(self, model, fsdp):
        return {"model": model, "fsdp": fsdp}

    def along_z(self, down):
        return self.below if down else self.above

    def has(self, down):
        return self.has_below if down else self.has_above

    def index(self, z, flip_y, flip_x, flip_core):
        flipped = lambda at, flip: 1 - at if flip else at
        return ((z * 2 + flipped(self.y, flip_y)) * 2 + flipped(self.x, flip_x)) * 2 + flipped(self.core, flip_core)

    def meet(self):
        barrier = pltpu.get_barrier_semaphore()

        def greet(other):
            pl.semaphore_signal(barrier, inc=1, device_id=other, device_id_type=pl.DeviceIdType.MESH)

        for other in (self.over_y, self.over_x, self.over_core):
            greet(other)
        for down in PAIR:
            pl.when(self.has(down))(lambda: greet(self.along_z(down)))
        pl.semaphore_wait(barrier, 3 + self.has_above + self.has_below)


def remote(src, dst, sems, device):
    send_sem, recv_sem = sems
    return pltpu.make_async_remote_copy(src_ref=src, dst_ref=dst, send_sem=send_sem, recv_sem=recv_sem, device_id=device, device_id_type=pl.DeviceIdType.MESH)


GATHER_SEMS = [DMA((2, DEVICES)), DMA((2,)), DMA((3, 2, DEPTH, 2)), DMA((2, 2, DEPTH, 2))]


def gather_all(at, own, out, recv, send_first, send_third, send_core):
    across = lambda k, third: at.over_x if k ^ third ^ 1 == 0 else at.over_y

    def landed(k, r):
        remote(own.at[k], out.at[r, k], (send_first.at[k], recv.at[k, r]), at.over_core).wait_recv()

    def index(k, z, j, third, core):
        return at.index(z, third if k else j, j if k else third, core)

    def walk(begin):
        def send(k, r, src, sem, device):
            c = remote(src, out.at[r, k], (sem, recv.at[k, r]), device)
            (c.start if begin else c.wait_send)()

        def spread(k, z, j, onward, src=None):
            r = index(k, z, j, 0, 0)
            src = out.at[r, k] if src is None else src
            place = (z - at.z + DEPTH) % DEPTH
            for down in onward:
                pl.when(at.has(down))(lambda: send(k, r, src, send_third.at[down, k, place, j], at.along_z(down)))
            send(k, r, src, send_third.at[2, k, place, j], across(k, 1))
            send(k, r, src, send_core.at[0, k, place, j], at.over_core)

        me = index(0, at.z, 0, 0, 0)
        for k in PAIR:
            send(k, me, own.at[k], send_first.at[k], across(k, 0))
            spread(k, at.z, 0, PAIR, own.at[k])
        if begin:
            out[me] = own[...]
        for k in PAIR:
            if begin:
                landed(k, index(k, at.z, 1, 0, 0))
            spread(k, at.z, 1, PAIR)
        for s in AWAY:
            for down in PAIR:
                z = at.z + s if down else at.z - s

                @pl.when((z >= 0) & (z <= LAST_Z))
                def _():
                    for j in PAIR:
                        for k in PAIR:
                            if begin:
                                landed(k, index(k, z, j, 0, 0))
                            spread(k, z, j, (down,))

        for core in PAIR:
            for s in range(DEPTH):
                z = (at.z + s) % DEPTH
                for j in PAIR:
                    for k in PAIR:
                        for third in PAIR if core else (1,):
                            r = index(k, z, j, third, core)
                            if begin:
                                landed(k, r)
                            if not core:
                                send(k, r, out.at[r, k], send_core.at[1, k, s, j], at.over_core)

    walk(True)
    walk(False)


def scatter_scratch(block, width, dtype):
    half = (block // 2, width)
    shapes = ((CHIPS, 2), (CHIPS, 2), (2, DEPTH, 2), (2, 2, DEPTH, 2), (2,))
    sems = ((2, CHIPS), (2, 2, DEPTH, 2), (2, 2, 2, DEPTH, 2), (2, 2))
    return [VMEM(s + half, dtype) for s in shapes] + [DMA(s) for s in sems]


def scatter_sum(at, part, out, sums, from_core, from_third, from_z, from_first, core_sem, third_sem, z_sem, first_sem, hook=lambda point: None):
    slot = lambda z, dy, dx: (z * 2 + dy) * 2 + dx
    near = lambda k, z, j: slot(z, 0, j) if k else slot(z, j, 0)
    far = lambda k, z, j: slot(z, 1, j) if k else slot(z, j, 1)
    both = lambda sem, *where: (sem.at[(0, *where)], sem.at[(1, *where)])

    def over_chip(z, dy, dx):
        s = slot(z, dy, dx)
        return remote(part.at[at.index(z, dy, dx, 1)], from_core.at[s], both(core_sem, s), at.over_core)

    def over_third(k, z, j):
        return remote(sums.at[far(k, z, j), k], from_third.at[k, z, j], both(third_sem, k, z, j), at.over_y if k else at.over_x)

    def along(down, k, z, j):
        return remote(sums.at[near(k, z, j), k], from_z.at[down, k, z, j], both(z_sem, down, k, z, j), at.along_z(down))

    def last(k):
        return remote(sums.at[near(k, at.z, 1), k], from_first.at[k], both(first_sem, k), at.over_x if k else at.over_y)

    def add(k, z, j, more):
        sums[near(k, z, j), k] = sums[near(k, z, j), k] + more

    def add_from_z(down, z, onward):
        for j in PAIR:
            for k in PAIR:
                along(down, k, z, j).wait_recv()
                add(k, z, j, from_z[down, k, z, j])
                if onward:
                    along(down, k, z, j).start()

    for z in FAR_FIRST:
        for dy, dx in SIDES:
            over_chip(z, dy, dx).start()
    for z in FAR_FIRST:
        for dy, dx in SIDES:
            s = slot(z, dy, dx)
            over_chip(z, dy, dx).wait_recv()
            sums[s] = part[at.index(z, dy, dx, 0)] + from_core[s]
            if dx:
                over_third(0, z, dy).start()
            if dy:
                over_third(1, z, dx).start()
    hook(0)
    for z in FAR_FIRST:
        for j in PAIR:
            for k in PAIR:
                over_third(k, z, j).wait_recv()
                add(k, z, j, from_third[k, z, j])
                pl.when((at.z == 0) & (z > 0))(lambda: along(0, k, z, j).start())
                pl.when((at.z == LAST_Z) & (z < LAST_Z))(lambda: along(1, k, z, j).start())
    for point, z in enumerate(FAR_FIRST):
        hook(1 + point)
        pl.when((at.z > 0) & (at.z < z))(lambda: add_from_z(0, z, True))
        pl.when((at.z < LAST_Z) & (at.z > z))(lambda: add_from_z(1, z, True))
    hook(1 + DEPTH)
    for down in PAIR:
        pl.when(at.has(not down))(lambda: add_from_z(down, at.z, False))
    for k in PAIR:
        last(k).start()
    for k in PAIR:
        last(k).wait_recv()
        out[k] = sums[near(k, at.z, 0), k] + from_first[k]
        last(k).wait_send()
    for z in FAR_FIRST:
        for dy, dx in SIDES:
            over_chip(z, dy, dx).wait_send()
        for j in PAIR:
            for k in PAIR:
                over_third(k, z, j).wait_send()
                pl.when(at.z < z)(lambda: along(0, k, z, j).wait_send())
                pl.when(at.z > z)(lambda: along(1, k, z, j).wait_send())


CHUNKS = 7
WEIGHT_SEMS = [DMA((2,)), DMA((2, 2)), DMA((2, CHUNKS)), DMA((2, CHUNKS)), DMA((2, 2, CHUNKS))]


class Weights:
    def __init__(self, at, shards, staged, wholes, local_sem, own_sem, x_sem, y_sem, core_sem):
        self.at, self.shards, self.staged, self.wholes = at, shards, staged, wholes
        self.local_sem, self.own_sem, self.x_sem, self.y_sem, self.core_sem = local_sem, own_sem, x_sem, y_sem, core_sem
        self.across = at.fsdp + 2 - DEPTH * at.x
        self.rows = shards[0].shape[0] // CHUNKS

    def either(self, copy_of, act):
        for y in PAIR:
            pl.when(self.at.y == y)(lambda: act(copy_of(y)))

    def chunk(self, i):
        return pl.ds(i * self.rows, self.rows)

    def local(self, w):
        return pltpu.make_async_copy(self.staged[w], self.wholes[w].at[self.at.fsdp], self.local_sem.at[w])

    def own(self, w):
        return remote(self.staged[w], self.wholes[w].at[self.at.fsdp], (self.own_sem.at[0, w], self.own_sem.at[1, w]), self.at.over_core)

    def over_x(self, i):
        sems = self.x_sem.at[0, i], self.x_sem.at[1, i]
        return lambda y: remote(self.shards[y].at[self.chunk(i)], self.wholes[y].at[self.at.fsdp, self.chunk(i)], sems, self.at.over_x)

    def onward(self, i, sem, device, other=False):
        sems = sem.at[0, i], sem.at[1, i]

        def copy(y):
            where = self.wholes[1 - y if other else y].at[self.across, self.chunk(i)]
            return remote(where, where, sems, device)

        return copy

    def over_y(self, i, other=False):
        return self.onward(i, self.y_sem, self.at.over_y, other)

    def over_core(self, other, i):
        return self.onward(i, self.core_sem.at[other], self.at.over_core, other)

    def start(self):
        for w in PAIR:
            self.own(w).start()
            self.local(w).start()
        self.send(0)

    def send(self, i):
        self.either(self.over_x(i), lambda c: c.start())

    def pass_on(self, i):
        self.either(self.over_x(i), lambda c: c.wait_recv())
        self.either(self.over_y(i), lambda c: c.start())
        self.either(self.over_core(0, i), lambda c: c.start())

    def hook(self, point):
        if point:
            self.pass_on(point - 1)
        else:
            for i in range(1, CHUNKS):
                self.send(i)

    def finish(self, passed):
        for i in range(passed, CHUNKS):
            self.pass_on(i)
        for i in range(CHUNKS):
            self.either(self.over_y(i, True), lambda c: c.wait_recv())
            self.either(self.over_core(1, i), lambda c: c.start())
        for w in PAIR:
            self.local(w).wait()
            self.own(w).wait()
        for i in range(CHUNKS):
            self.either(self.over_x(i), lambda c: c.wait_send())
            self.either(self.over_y(i), lambda c: c.wait_send())
            for other in PAIR:
                self.either(self.over_core(other, i), lambda c: c.wait())


def gather_rows(ids, ids_wide, base, table, table_tail):
    total = ids.shape[0]
    rows, width = table.shape
    groups = total // LANES
    depth, group = 64, 16
    last_block = rows // SUBLANES * SUBLANES

    def kernel(ids_ref, wide_ref, base_ref, table_ref, tail_ref, out_ref, token, listed, held, list_sem, in_sem):
        start_row = base_ref[0]
        local = wide_ref[...] - start_row
        owned = ((local >= 0) & (local < rows)).astype(F32)
        square, tall = (LANES, LANES), (groups, groups)
        within = matmul(owned, (iota(square, 0) <= iota(square, 1)).astype(F32))
        count = within[:, LANES - 1 :]
        earlier = matmul((iota(tall, 1) < iota(tall, 0)).astype(F32), jnp.broadcast_to(count, local.shape))
        rank = jnp.where(owned > 0, earlier + within - 1, -1.0).astype(jnp.int32)
        which = jnp.zeros((groups, LANES), F32)
        lane = iota((1, LANES), 1)
        for g in range(groups):
            r = rank[g : g + 1, :]
            column = (iota(square, 0) == jnp.where(r < 0, -1, r % LANES)).astype(F32)
            row = (iota((groups, LANES), 0) == jnp.where(r < 0, -1, r // LANES)).astype(F32)
            which += matmul_nt(row * (lane + 1).astype(F32), column) + matmul_nt(row * float(g * LANES), column)
        listed[:groups, :] = which.astype(jnp.int32) - 1
        filled_wide = earlier[groups - 1 :, :] + jnp.broadcast_to(count[groups - 1 :, :], (1, LANES))
        listed[groups:, :] = jnp.broadcast_to(filled_wide, (SUBLANES, LANES)).astype(jnp.int32)
        copy = pltpu.make_async_copy(listed, token, list_sem)
        copy.start()
        copy.wait()
        filled = token[groups, 0]

        def token_of(j):
            return token[j // LANES, j % LANES]

        def row_of(j):
            return ids_ref[token_of(j)] - start_row

        def block_copy(j):
            block = jnp.minimum(row_of(j) // SUBLANES, last_block // SUBLANES - 1)
            return pltpu.make_async_copy(table_ref.at[rows_at(block, SUBLANES)], held.at[j % depth], in_sem.at[j % depth])

        repeat(jnp.minimum(filled, depth), lambda j: block_copy(j).start())

        def clear(i):
            out_ref[rows_at(i, depth), :] = jnp.zeros((depth, width), BF)

        repeat(total // depth, clear)
        sublane, sublane_out = iota((SUBLANES, width), 0), iota((group, width), 0)

        def step(j):
            block_copy(j).wait()
            t, row = token_of(j), row_of(j)
            in_tail = row >= last_block
            chosen = jnp.where(in_tail, row - (rows - SUBLANES), row % SUBLANES)
            block = jnp.where(in_tail, tail_ref[...].astype(F32), held[j % depth].astype(F32))
            picked = jnp.sum(jnp.where(sublane == chosen, block, 0.0), axis=0, keepdims=True)
            where = rows_at(t // group, group)
            out_ref[where, :] = jnp.where(sublane_out == t % group, picked, out_ref[where, :].astype(F32)).astype(BF)
            pl.when(j + depth < filled)(lambda: block_copy(j + depth).start())

        repeat(filled, step)

    listing = (groups + SUBLANES, LANES)
    return pl.pallas_call(
        kernel,
        out_shape=(jax.ShapeDtypeStruct((total, width), BF), jax.ShapeDtypeStruct(listing, jnp.int32)),
        in_specs=[IN_SMEM, IN_VMEM, IN_SMEM, IN_PLACE, IN_VMEM],
        out_specs=(IN_VMEM, IN_SMEM),
        scratch_shapes=[VMEM(listing, jnp.int32), VMEM((depth, SUBLANES, width), BF), DMA, DMA((depth,))],
        cost_estimate=pl.CostEstimate(flops=total * total * width, bytes_accessed=total * width, transcendentals=0),
        name="gather_rows",
    )(ids, ids_wide, base, table, table_tail)


def add_rows(token, ids, base, values, grad, rows):
    total, width = values.shape
    block_rows = 512
    blocks = pl.cdiv(rows, block_rows)

    def kernel(token, ids_ref, base_ref, values_ref, grad_ref, out_ref, head, following, held, sem):
        block = pl.program_id(0)
        fetch = pltpu.make_async_copy(values_ref, held.at[pl.ds(0, total)], sem)
        token_of = lambda j: token[j // LANES, j % LANES]

        @pl.when(block == 0)
        def _():
            fetch.start()

            def clear(b):
                head[b] = -1

            def chain(j):
                owner = (ids_ref[token_of(j)] - base_ref[0]) // block_rows
                following[j] = head[owner]
                head[owner] = j

            repeat(blocks, clear)
            repeat(token[total // LANES, 0], chain)
            fetch.wait()

        out_ref[...] = grad_ref[...]
        sublane = iota((SUBLANES, width), 0)

        def add(j):
            t = token_of(j)
            row = ids_ref[t] - base_ref[0] - block * block_rows
            where = rows_at(row // SUBLANES, SUBLANES)
            out_ref[where, :] += jnp.where(sublane == row % SUBLANES, held[pl.ds(t, 1), :], 0.0)
            return following[j]

        lax.while_loop(lambda j: j >= 0, add, head[block])

    block_spec = pl.BlockSpec((block_rows, width), lambda i: (i, 0))
    in_smem = pltpu.MemorySpace.SMEM
    return pl.pallas_call(
        kernel,
        grid=(blocks,),
        out_shape=jax.ShapeDtypeStruct((rows, width), F32),
        in_specs=[IN_SMEM, IN_SMEM, IN_SMEM, IN_PLACE, block_spec],
        out_specs=block_spec,
        scratch_shapes=[in_smem((blocks,), jnp.int32), in_smem((total,), jnp.int32), VMEM((total + SUBLANES, width), F32), DMA],
        cost_estimate=pl.CostEstimate(flops=total * total * width, bytes_accessed=rows * width, transcendentals=0),
        name="add_rows",
    )(token, ids, base, values, grad)


def front(part, *shards):
    total, width = part.shape
    block = total // DEVICES
    shape = (2, block // 2, width)
    scratch = scatter_scratch(block, width, BF)

    def kernel(part_ref, gate_ref, up_ref, gate_in, up_in, x_ref, gate_out, up_out, *rest):
        at = Place()
        at.meet()
        weights = Weights(at, (gate_ref, up_ref), (gate_in, up_in), (gate_out, up_out), *rest[len(scratch) :])
        weights.start()
        scatter_sum(at, part_ref, x_ref, *rest[: len(scratch)], hook=weights.hook)
        weights.finish(DEPTH + 1)

    x, *wholes = pl.pallas_call(
        kernel,
        out_shape=[jax.ShapeDtypeStruct(s, BF) for s in (shape, *((DEPTH,) + w.shape for w in shards))],
        in_specs=[IN_VMEM] + [IN_PLACE] * 2 + [IN_VMEM] * 2,
        out_specs=[IN_VMEM] + [IN_PLACE] * 2,
        scratch_shapes=scratch + WEIGHT_SEMS,
        compiler_params=pltpu.CompilerParams(collective_id=0, has_side_effects=True),
        name="front",
    )(part.reshape(DEVICES, *shape), *shards, *shards)
    return x.reshape(block, width), *(w.reshape(-1, w.shape[2]) for w in wholes)


def all_blocks(own, collective_id):
    block, width = own.shape
    shape = (2, block // 2, width)

    def kernel(own_ref, out_ref, *sems):
        at = Place()
        at.meet()
        gather_all(at, own_ref, out_ref, *sems)

    return pl.pallas_call(
        kernel,
        out_shape=jax.ShapeDtypeStruct((DEVICES,) + shape, own.dtype),
        in_specs=[IN_VMEM],
        out_specs=IN_VMEM,
        scratch_shapes=GATHER_SEMS,
        compiler_params=pltpu.CompilerParams(collective_id=collective_id, has_side_effects=True),
        name="all_blocks",
    )(own.reshape(shape)).reshape(DEVICES, block, width)


TILE = 2 * LANES


def head_forward(hn_t, table, table_end, label_at):
    homes, width, _ = hn_t.shape
    rows = table.shape[0]
    inside = rows // SUBLANES * SUBLANES
    padded = inside + table_end.shape[0]
    tiles = padded // TILE
    parts = 4
    chunk = padded // parts

    def kernel(hn_ref, table_ref, end_ref, label_ref, z_ref, stats_ref, turned_ref, held, sem):
        step = pl.program_id(0)

        @pl.when(step == 0)
        def _():
            held[inside:, :] = end_ref[...]
            copy = pltpu.make_async_copy(table_ref.at[pl.ds(0, inside)], held.at[pl.ds(0, inside)], sem)
            copy.start()
            copy.wait()

        tokens = jnp.concatenate([hn_ref[h] for h in PAIR], axis=1)
        grouped = lambda t: t.reshape(chunk // SUBLANES, SUBLANES, TILE)
        most = jnp.full((SUBLANES, TILE), -jnp.inf, F32)
        summed = label_sum = jnp.zeros((SUBLANES, TILE), F32)
        for c in range(parts):
            where = pl.ds(c * chunk, chunk)
            row = iota((chunk, TILE), 0) + c * chunk
            z = matmul(held[where, :], tokens)
            if c * chunk + chunk > rows:
                z = jnp.where(row < rows, z, -jnp.inf)
            z_ref[where, :] = z
            now = jnp.maximum(most, jnp.max(grouped(z), axis=0))
            summed = summed * jnp.exp(most - now) + jnp.sum(jnp.exp(grouped(z) - now), axis=0)
            label_sum += jnp.sum(grouped(jnp.where(row == label_ref[...], z, 0.0)), axis=0)
            most = now
        peak = jnp.max(most, axis=0, keepdims=True)
        total_exp = jnp.sum(summed * jnp.exp(most - peak), axis=0, keepdims=True)
        label_z = jnp.sum(label_sum, axis=0, keepdims=True)
        line = iota((SUBLANES, TILE), 0)
        stats = jnp.where(line == 0, peak, jnp.where(line == 1, total_exp, label_z))
        for h in PAIR:
            stats_ref[h] = stats[:, h * LANES : (h + 1) * LANES]

        def turn(tile):
            turned_ref[:, rows_at(tile, TILE)] = held[rows_at(tile, TILE), :].T

        for tile in (step, step + CHIPS):
            pl.when(tile < tiles)(lambda: turn(tile))

    stats = jax.ShapeDtypeStruct((homes, SUBLANES, LANES), F32)
    return pl.pallas_call(
        kernel,
        grid=(CHIPS,),
        out_shape=(jax.ShapeDtypeStruct((CHIPS, padded, TILE), F32), stats, jax.ShapeDtypeStruct((width, padded), BF)),
        in_specs=[pl.BlockSpec((2, width, LANES), lambda i: (i, 0, 0)), IN_PLACE, whole(table_end), pl.BlockSpec((None, 1, TILE), lambda i: (i, 0, 0))],
        out_specs=(
            pl.BlockSpec((None, padded, TILE), lambda i: (i, 0, 0)),
            pl.BlockSpec((2, SUBLANES, LANES), lambda i: (i, 0, 0)),
            pl.BlockSpec((width, padded), lambda i: (0, 0), pipeline_mode=pl.Buffered(1)),
        ),
        scratch_shapes=[VMEM((padded, width), BF), DMA],
        cost_estimate=pl.CostEstimate(flops=2 * homes * LANES * rows * width, bytes_accessed=4 * homes * LANES * rows, transcendentals=homes * LANES * rows),
        name="head_forward",
    )(hn_t, table, table_end, label_at)


def head_backward(logits, stats, label_at, hn_t, table_t):
    padded, total = logits.shape[1], CHIPS * TILE
    width = table_t.shape[0]
    half = (width // 2, LANES)
    step_rows = 512
    starts = range(0, padded, step_rows)

    def kernel(z_ref, stats_ref, label_ref, hn_ref, table_ref, head_ref, out_ref, z_in, hn_in, dz, dhn, sums, from_third, from_z, from_first, z_sem, hn_sem, core_sem, third_sem, up_sem, down_sem, first_sem):
        at = Place()
        low = at.z < 2
        both = lambda sem, *where: (sem.at[(0, *where)], sem.at[(1, *where)])

        def target(g):
            near = jnp.where(low, jnp.where(g < 2, LAST_Z - g, 1 - at.z), jnp.where(g < 2, g, LAST_Z + 2 - at.z))
            return jnp.where(g == LAST_Z, at.z, near)

        def chip(i):
            q = i % DEPTH
            return target(i // DEPTH), 1 - q % 2, 1 - q // 2

        def slot(z, dy, dx):
            return (z * 2 + dy) * 2 + dx

        def block_of(i):
            z, dy, dx = chip(i)
            y = at.y + dy - 2 * dy * at.y
            x = at.x + dx - 2 * dx * at.x
            return (z * 2 + y) * 2 + x

        def near(k, z, j):
            return slot(z, 0, j) if k else slot(z, j, 0)

        def load(i):
            s, b = i % 2, block_of(i)
            return (
                pltpu.make_async_copy(z_ref.at[b], z_in.at[s], z_sem.at[s]),
                pltpu.make_async_copy(hn_ref.at[rows_at(b, 2)], hn_in.at[s], hn_sem.at[s]),
            )

        def begin(i):
            for c in load(i):
                c.start()

        def over_chip(i):
            s = slot(*chip(i))
            return remote(dhn.at[i % 2, 1 - at.core], sums.at[s], both(core_sem, s), at.over_core)

        def over_third(k, z, j):
            far = slot(z, 1, j) if k else slot(z, j, 1)
            return remote(sums.at[far, k], from_third.at[k, z, j], both(third_sem, k, z, j), at.over_y if k else at.over_x)

        def along(down, k, z, j):
            sem = down_sem if down else up_sem
            return remote(sums.at[near(k, z, j), k], from_z.at[down, k, z, j], both(sem, k, z, j), at.along_z(down))

        def last(k):
            return remote(sums.at[near(k, at.z, 1), k], from_first.at[k], both(first_sem, k), at.over_x if k else at.over_y)

        def add(k, z, j, more):
            sums[near(k, z, j), k] += more

        def each(act):
            for j in PAIR:
                for k in PAIR:
                    act(k, j)

        def compute(i):
            s, b = i % 2, block_of(i)
            for c in load(i):
                c.wait()
            pl.when(i + 1 < CHIPS)(lambda: begin(i + 1))
            pair = lambda line: jnp.concatenate([stats_ref[2 * b + h][line : line + 1, :] for h in PAIR], axis=1)
            peak, inverse = pair(0), pair(1) / total
            tokens = jnp.concatenate([hn_in[s, h] for h in PAIR], axis=1)
            for first in starts:
                where = pl.ds(first, min(step_rows, padded - first))
                soft = jnp.exp(z_in[s, where, :] - peak) * inverse
                dz[where, :] = (soft - jnp.where(iota(soft.shape, 0) + first == label_ref[b], 1.0 / total, 0.0)).astype(BF)
                product = matmul(table_ref[:, where], dz[where, :])
                for h in PAIR:
                    part = product[:, h * LANES : (h + 1) * LANES].reshape(2, *half)
                    dhn[s, h] = dhn[s, h] + part if first else part
                head_ref[where, :] += matmul_nt(dz[where, :], tokens)

        def join(i):
            c = over_chip(i)
            c.wait()
            z, dy, dx = chip(i)
            s = slot(z, dy, dx)
            sums[s] += dhn[i % 2, at.core]
            pl.when(dx == 1)(lambda: over_third(0, z, dy).start())
            pl.when(dy == 1)(lambda: over_third(1, z, dx).start())

        def third(g):
            z = target(g)

            def receive(k, j):
                over_third(k, z, j).wait()
                add(k, z, j, from_third[k, z, j])
                pl.when((at.z == 0) & (z > 0))(lambda: along(0, k, z, j).start())
                pl.when((at.z == LAST_Z) & (z < LAST_Z))(lambda: along(1, k, z, j).start())

            each(receive)

        def relay(g):
            z = target(g)
            for down in PAIR:

                def pass_on(k, j):
                    along(down, k, z, j).wait_recv()
                    add(k, z, j, from_z[down, k, z, j])
                    along(down, k, z, j).start()

                pl.when((at.z < LAST_Z) & (z < at.z) if down else (at.z > 0) & (z > at.z))(lambda: each(pass_on))

        at.meet()
        begin(0)
        head_ref[...] = jnp.zeros_like(head_ref)

        def step(i):
            compute(i)
            over_chip(i).start()
            g = i // DEPTH - 1
            pl.when(i > 0)(lambda: join(i - 1))
            pl.when((g >= 0) & (i % DEPTH == 1))(lambda: third(g))
            pl.when((g >= 0) & (i % DEPTH == 2))(lambda: relay(g))

        repeat(CHIPS, step)
        join(CHIPS - 1)
        third(LAST_Z)
        for down in PAIR:

            def arrive(k, j):
                along(down, k, at.z, j).wait_recv()
                add(k, at.z, j, from_z[down, k, at.z, j])

            pl.when(at.has(not down))(lambda: each(arrive))
        for k in PAIR:
            last(k).start()
        for k in PAIR:
            last(k).wait()
            out_ref[k] = sums[near(k, at.z, 0), k] + from_first[k]
        for z in range(DEPTH):
            for down in PAIR:
                pl.when(at.z > z if down else at.z < z)(lambda: each(lambda k, j: along(down, k, z, j).wait_send()))

    twice = (2, DEPTH, 2)
    buffers = (((2, padded, TILE), F32), ((2, 2, width, LANES), BF), ((padded, TILE), BF)) + tuple(
        (s + half, F32) for s in ((2, 2, 2), (CHIPS, 2), twice, (2,) + twice, (2,))
    )
    sems = ((2,), (2,), (2, CHIPS), (2,) + twice, (2,) + twice, (2,) + twice, (2, 2))
    return pl.pallas_call(
        kernel,
        out_shape=(jax.ShapeDtypeStruct((padded, width), F32), jax.ShapeDtypeStruct((2,) + half, F32)),
        in_specs=[IN_PLACE, IN_VMEM, IN_VMEM, IN_PLACE, IN_VMEM],
        out_specs=(IN_VMEM, IN_VMEM),
        scratch_shapes=[VMEM(*b) for b in buffers] + [DMA(s) for s in sems],
        compiler_params=pltpu.CompilerParams(collective_id=3, has_side_effects=True, vmem_limit_bytes=67_000_000),
        cost_estimate=pl.CostEstimate(flops=4 * total * padded * width, bytes_accessed=4 * total * padded, transcendentals=total * padded),
        name="head_backward",
    )(logits, stats, label_at, hn_t, table_t)


def combine_stats(local):
    homes = local.shape[0]

    def kernel(local_ref, out_ref, inbox, mine, to_home, at_home, to_all, from_all):
        me = lax.axis_index("model") * DEPTH + lax.axis_index("fsdp")

        def device(s):
            r = (me + s) % homes
            return r, {"model": r // DEPTH, "fsdp": r % DEPTH}

        def first(s):
            r, other = device(s)
            return remote(local_ref.at[r], inbox.at[s], (to_home.at[s], at_home.at[s]), other)

        def second(s, sender):
            return remote(mine, out_ref.at[sender], (to_all.at[s], from_all.at[s]), device(s)[1])

        others = range(1, homes)
        for s in others:
            first(s).start()
        inbox[0] = local_ref[me]
        for s in others:
            first(s).wait()
        peaks = inbox[:, 0, :]
        peak = jnp.max(peaks, axis=0, keepdims=True)
        total_exp = jnp.sum(inbox[:, 1, :] * jnp.exp(peaks - peak), axis=0, keepdims=True)
        label_z = jnp.sum(inbox[:, 2, :], axis=0, keepdims=True)
        row = iota((SUBLANES, LANES), 0)
        mine[...] = jnp.where(row == 0, peak, jnp.where(row == 1, 1.0 / total_exp, jnp.where(row == 2, label_z, total_exp)))
        for s in others:
            second(s, me).start()
        out_ref[me] = mine[...]
        for s in others:
            second(s, me).wait_send()
            second(s, (me + homes - s) % homes).wait_recv()

    return pl.pallas_call(
        kernel,
        out_shape=jax.ShapeDtypeStruct(local.shape, F32),
        in_specs=[IN_VMEM],
        out_specs=IN_VMEM,
        scratch_shapes=[VMEM((homes, SUBLANES, LANES), F32), VMEM((SUBLANES, LANES), F32)] + [DMA((homes,))] * 4,
        compiler_params=pltpu.CompilerParams(has_side_effects=True),
        name="combine_stats",
    )(local)


def weight_grads(side, a, a_chip_t, dm, dm_t, w_gate, w_up, w_down):
    tokens, width = a.shape
    chip_rows = a_chip_t.shape[0]
    hidden = w_gate.shape[1]
    tiles = hidden // TILE
    kept = tiles // 2 + 1
    chunk = tokens // 4

    def kernel(side_ref, a_ref, a_chip_ref, dm_ref, dm_t_ref, gate_ref, up_ref, down_ref, grad_gate, grad_up, grad_down, act, d_gate, d_up):
        def some(i):
            where = rows_at(i, chunk)
            gate_f = matmul(a_ref[where, :], gate_ref[...]).astype(BF).astype(F32)
            up_f = matmul(a_ref[where, :], up_ref[...]).astype(BF).astype(F32)
            d_act = matmul_nt(dm_ref[where, :], down_ref[...])
            sig = jax.nn.sigmoid(gate_f)
            silu = gate_f * sig
            act[where, :] = (silu * up_f).astype(BF)
            d_gate[where, :] = (d_act * up_f * (sig * (1.0 + gate_f * (1.0 - sig)))).astype(BF)
            d_up[where, :] = (d_act * silu).astype(BF)

        repeat(tokens // chunk, some)
        grad_gate[...] = matmul(a_chip_ref[...], d_gate[...])
        grad_up[...] = matmul(a_chip_ref[...], d_up[...])
        at = pl.program_id(0) - side_ref[0] * (kept - 1)

        @pl.when((at >= 0) & (at < kept))
        def _():
            grad_down[...] = matmul(dm_t_ref[...], act[...]).T

    columns = lambda n: pl.BlockSpec((n, TILE), lambda i, side: (0, i))
    return pl.pallas_call(
        kernel,
        grid_spec=pltpu.PrefetchScalarGridSpec(
            num_scalar_prefetch=1,
            grid=(tiles,),
            in_specs=[whole(a), whole(a_chip_t), whole(dm), whole(dm_t), columns(width), columns(width), pl.BlockSpec((TILE, width), lambda i, side: (i, 0))],
            out_specs=[columns(chip_rows), columns(chip_rows), pl.BlockSpec((TILE, width), lambda i, side: (jnp.clip(i - side[0] * (kept - 1), 0, kept - 1), 0))],
            scratch_shapes=[VMEM((tokens, TILE), BF)] * 3,
        ),
        out_shape=[jax.ShapeDtypeStruct(s, F32) for s in ((chip_rows, hidden), (chip_rows, hidden), (kept * TILE, width))],
        cost_estimate=pl.CostEstimate(flops=9 * tokens * hidden * width, bytes_accessed=6 * hidden * width, transcendentals=tokens * hidden),
        name="weight_grads",
    )(side, a, a_chip_t, dm, dm_t, w_gate, w_up, w_down)


def solution(mesh):
    row_spec = P(ALL, None)
    fsdp_spec = P("fsdp", None)

    def device_step(tok_ids, tok_labels, table, gate_shard, up_shard, down_shard, gain_in, gain_out):
        fsdp_at = lax.axis_index("fsdp")
        core, side = fsdp_at % 2, fsdp_at // 2
        num_tokens = tok_ids.size * DEPTH
        rows, width = table.shape
        first_row = (lax.axis_index("model") * DEPTH + fsdp_at) * rows
        inside = rows // SUBLANES * SUBLANES

        both = jnp.stack([tok_ids.reshape(-1), tok_labels.reshape(-1)])
        both = lax.all_gather(both, "fsdp", axis=1, tiled=True)
        ids, labels = both[0], both[1]
        base = first_row.reshape(1)
        w_down = lax.all_gather(down_shard, "fsdp", axis=0, tiled=True)
        part, token = gather_rows(ids, ids.reshape(-1, LANES), base, table, table[rows - SUBLANES :])
        x_bf, w_gate, w_up = front(part, gate_shard, up_shard)

        h_res, (norm_in_back, a_mine, gate_f, up_f, gate_sig, silu_gate) = mlp_forward(x_bf.astype(F32), gain_in, w_gate, w_up, w_down)
        hn_f, norm_out_back = jax.vjp(lambda values: rms_scale(values, gain_out), h_res)
        hn_t = all_blocks(hn_f.astype(BF).T, 1)
        hn_t, a_mine = lax.optimization_barrier((hn_t, a_mine))
        a_all = lax.all_gather(a_mine, ALL, axis=0, tiled=True)

        label_at = labels - first_row
        label_at = jnp.where((label_at >= 0) & (label_at < rows), label_at, -1).reshape(CHIPS, 1, TILE)
        table_end = jnp.pad(table[inside:], ((0, pl.cdiv(rows, TILE) * TILE - rows), (0, 0)))
        logits, local_stats, table_t = head_forward(hn_t, table, table_end, label_at)
        stats = combine_stats(local_stats)
        loss = jnp.sum(stats[:, 0, :] + jnp.log(stats[:, 3, :]) - stats[:, 2, :]) / num_tokens
        d_head, d_hn_t = head_backward(logits, stats, label_at, hn_t, table_t)
        d_hn_t, a_all = lax.optimization_barrier((d_hn_t, a_all))
        d_hn = d_hn_t.reshape(width, -1).T

        d_hidden = norm_out_back(d_hn)[0]
        d_mlp = d_hidden.astype(BF)
        ours = lambda t: lax.dynamic_index_in_dim(t.reshape(CHIPS, 2, -1, width), core, axis=1, keepdims=False).reshape(-1, width)
        dm_all = all_blocks(d_mlp, 2)
        dm_half = ours(dm_all)
        d_act = matmul_nt(d_mlp, w_down)
        d_gate = (d_act * up_f * (gate_sig * (1.0 + gate_f * (1.0 - gate_sig)))).astype(BF)
        d_up = (d_act * silu_gate).astype(BF)
        d_x = d_hidden + norm_in_back(matmul_nt(d_gate, w_gate) + matmul_nt(d_up, w_up))[0]
        d_x, dm_all = lax.optimization_barrier((d_x, dm_all))
        d_x_all = lax.all_gather(d_x, ALL, axis=0, tiled=True)

        a_half = ours(a_all)
        chip_rows = width // 2
        a_chip_t = lax.dynamic_slice(a_half, (0, side * chip_rows), (num_tokens // 2, chip_rows)).T
        grads = list(weight_grads(side.reshape(1), a_half, a_chip_t, dm_half, dm_half.T, w_gate, w_up, w_down))
        hidden_rows = down_shard.shape[0] * 2
        grads[2] = lax.dynamic_slice(grads[2], (side * (grads[2].shape[0] - hidden_rows), 0), (hidden_rows, width))
        swap = [(i, i ^ 1) for i in range(DEPTH)]

        def share(grad):
            grad = grad.reshape(2, -1, grad.shape[1])
            part_of = lambda c: lax.dynamic_index_in_dim(grad, c, axis=0, keepdims=False)
            return part_of(core) + lax.ppermute(part_of(1 - core), "fsdp", swap)

        return loss, add_rows(token, ids, base, d_x_all, d_head, rows), *map(share, grads)

    in_specs = (fsdp_spec, fsdp_spec, row_spec, fsdp_spec, fsdp_spec, fsdp_spec, P(), P())
    return jax.shard_map(device_step, mesh=mesh, in_specs=in_specs, out_specs=(P(), row_spec, fsdp_spec, fsdp_spec, fsdp_spec), check_vma=False)
```
